32 devices in a mesh: groups: 2 (over x), shard: 16 (over z, y, core).
Axes of the slice: x: 2, y: 2, z: 4, core: 2. Of those that a mesh axis runs over, the one named last changes fastest.
Arguments:
- echoes: float32 [1, 2, 4, 512, 8192], P(None, None, 'groups', 'shard'), parts along dimension 2, may hold values from -6 to 6
- waveform: float32 [2, 8192], replicated, may hold values from -6 to 6
- doppler_taper: float32 [512], replicated, may hold values from 0.3 to 1
- cfar_guard: int32 [4], P('groups'), parts along dimension 0, may hold values from 1 to 4, as said below
- cfar_train: int32 [4], P('groups'), parts along dimension 0, may hold values from 2 to 16
- noise_floor: float32 [4], P('groups'), parts along dimension 0, may hold values from 0.5 to 2
Outputs:
- cfar_ratio: float32 [1, 4, 512, 8192], P(None, 'groups', None, 'shard'), parts along dimension 1
The draws below stay inside these ranges and needn't reach their ends.
There are 2 independent parts, one for each index of `groups`. The reference program is written for one: setup_inputs(seed, part) draws one part's arguments, and reference() takes and returns one part's arrays. A program takes and returns all parts, laid end to end along the dimension named above; an argument that names none is the same for every part. Nothing has to cross between parts.
Inputs may be any that keep to these rules, and one draw needn't show every extreme that they name: In every draw some beam has cfar_guard 4 together with cfar_train 16; no beam has more of either.
All inputs are finite; a program needn't handle non-finite values.
Results may differ from the reference program's by a relative error of at most 0.000075.
Values sent between devices are 32-bit elements; how exact they have to be, the bound alone decides.
A program may use at most 64 MiB of HBM per device.

```python
import math
import jax
import jax.numpy as jnp

NCPI = 1
BEAMS = 2
PULSES = 512
GATES = 8192
GUARD_MAX = 4
TRAIN_MAX = 16
HALO = 20


def cfar_windows(key):
    guard_key = jax.random.fold_in(key, 11)
    train_key = jax.random.fold_in(key, 12)
    pick_key = jax.random.fold_in(key, 13)
    guard_cells = jax.random.randint(guard_key, (BEAMS,), 1, GUARD_MAX + 1)
    train_cells = jax.random.randint(train_key, (BEAMS,), 2, TRAIN_MAX + 1)
    chosen = jax.random.randint(pick_key, (), 0, BEAMS)
    widest = jnp.arange(BEAMS) == chosen
    guard_cells = jnp.where(widest, GUARD_MAX, guard_cells)
    train_cells = jnp.where(widest, TRAIN_MAX, train_cells)
    return (guard_cells.astype(jnp.int32), train_cells.astype(jnp.int32))


def draw_cfar_guard(key, part):
    return cfar_windows(key)[0]


def draw_cfar_train(key, part):
    return cfar_windows(key)[1]


def block_scale(stream_key, dims, pieces, smallest, top_value):
    def one(axis_at, blocks):
        heights = jax.random.uniform(jax.random.fold_in(jax.random.fold_in(stream_key, 6), axis_at), (blocks,), jnp.float32, smallest / len(pieces), top_value / len(pieces))
        return jnp.repeat(jnp.exp(heights), dims[axis_at] // blocks).reshape((-1,) + (1,) * (len(dims) - axis_at - 1))

    level = one(*pieces[0])
    for cut in pieces[1:]:
        level = level * one(*cut)
    return level


def normal_values(stream_key, dims, width, reach, cuts=(), kind=jnp.bfloat16):
    level = block_scale(stream_key, dims, cuts, -0.22, 0.18) if cuts else 1.0
    result = jax.random.normal(stream_key, dims, jnp.float32) * width * level
    return jnp.minimum(jnp.maximum(result, -reach), reach).astype(kind)


def setup_inputs(seed: int = 0, part: int = 0) -> dict:
    key_list = jax.random.split(jax.random.key(seed), 7)
    part_keys = jax.random.split(jax.random.fold_in(key_list[6], part), 7)
    echoes = normal_values(part_keys[0], (NCPI, 2, BEAMS, PULSES, GATES), 1.0, 6.0, ((3, 16),), jnp.float32)
    waveform = normal_values(key_list[1], (2, GATES), 1.0, 6.0, (), jnp.float32)
    doppler_taper = jnp.clip(jnp.exp(jax.random.uniform(key_list[2], (PULSES,), jnp.float32, math.log(0.3), math.log(1.0))), 0.3, 1.0)
    cfar_guard = draw_cfar_guard(jax.random.fold_in(jax.random.fold_in(key_list[6], part), 71), part)
    cfar_train = draw_cfar_train(jax.random.fold_in(jax.random.fold_in(key_list[6], part), 71), part)
    noise_floor = jnp.clip(jnp.exp(jax.random.uniform(part_keys[5], (BEAMS,), jnp.float32, math.log(0.5), math.log(2.0))), 0.5, 2.0)
    return dict(echoes=echoes, waveform=waveform, doppler_taper=doppler_taper, cfar_guard=cfar_guard, cfar_train=cfar_train, noise_floor=noise_floor)


def reference(echoes, waveform, doppler_taper, cfar_guard, cfar_train, noise_floor):
    signal = echoes[:, 0] + 1j * echoes[:, 1]
    spectrum = jnp.fft.fft(signal, axis=-1)
    matched = waveform[0] - 1j * waveform[1]
    compressed = jnp.fft.ifft(spectrum * matched, axis=-1)
    tapered = compressed * doppler_taper[:, None]
    doppler = jnp.fft.fft(tapered, axis=2) / jnp.sqrt(jnp.float32(PULSES))
    power_map = jnp.real(doppler) ** 2 + jnp.imag(doppler) ** 2
    padded = jnp.pad(power_map, ((0, 0), (0, 0), (0, 0), (HALO, HALO)))
    offsets = jnp.arange(1, HALO + 1, dtype=jnp.int32)
    inside = (offsets[None, :] > cfar_guard[:, None]) & (offsets[None, :] <= (cfar_guard + cfar_train)[:, None])
    weights = inside.astype(jnp.float32)
    window_sum = jnp.zeros_like(power_map)
    for offset in range(1, HALO + 1):
        lower = padded[..., HALO - offset:HALO - offset + GATES]
        upper = padded[..., HALO + offset:HALO + offset + GATES]
        window_sum = window_sum + weights[:, offset - 1][None, :, None, None] * (lower + upper)
    noise_mean = window_sum / (2.0 * cfar_train.astype(jnp.float32))[None, :, None, None]
    return power_map / (noise_floor[None, :, None, None] + noise_mean)
```

```python
import functools
import math

import jax
import jax.numpy as jnp
import numpy as np
from jax import lax
from jax.experimental import pallas as pl
from jax.experimental.pallas import tpu as pltpu
from jax.sharding import PartitionSpec as P

GB = 128
ROWS = 8
EDGE = 24
MESH = pl.DeviceIdType.MESH


def split(table):
    table = np.asarray(table, np.float32)
    high = table.astype(jnp.bfloat16)
    low = (table - high.astype(np.float32)).astype(jnp.bfloat16)
    return high, low


def dft(length, size=None):
    size = size or length
    i = np.arange(size)[:, None] * np.arange(length)[None, :] % length
    angles = 2.0 * np.pi / length * i
    return np.cos(angles), np.sin(angles)


def tables(gates, pulses):
    ga = gates // GB
    ca, sa = dft(ga)
    cb, sb = dft(GB)

    def left(matrix):
        high, low = split(matrix)
        return np.block([[high, high], [low, np.zeros_like(low)]])

    def right(matrix):
        high, low = split(matrix)
        return np.concatenate([high, high, low], axis=0)

    first = left(np.block([[ca, sa], [-sa, ca]]))
    last = left(np.block([[ca, -sa], [sa, ca]]))
    second = right(np.block([[cb, -sb], [sb, cb]]))
    third = right(np.block([[cb, sb], [-sb, cb]]))
    i = np.arange(ga)[:, None] * np.arange(GB)[None, :] % gates
    twiddle = np.stack([np.cos(2 * np.pi / gates * i), np.sin(2 * np.pi / gates * i)])
    cp, sp = dft(pulses)
    high, low = split(np.concatenate([cp, sp], axis=0))
    doppler = np.concatenate([high, high, low], axis=1)
    return first, second, third, last, twiddle.astype(np.float32), doppler


def parts(x):
    high = x.astype(jnp.bfloat16)
    low = (x - high.astype(jnp.float32)).astype(jnp.bfloat16)
    return high, low


def dot(a, b):
    return jnp.dot(a, b, preferred_element_type=jnp.float32)


def kernel(
    n, beams, pulses, gates,
    echoes, filt, taper, guard, train, floor, first, second, third, last, twiddle, doppler_hbm,
    out,
    xin, xs, sent, got, table, rhs, spec, power, edge, halo, band, result,
    in_sem, table_sem, send_sem, recv_sem, edge_send, edge_recv, out_sem,
):
    me = lax.axis_index("shard")
    ga = gates // GB
    tiles = ga // n
    groups = pulses // n // ROWS
    order = sorted(range(1, n), key=lambda k: (abs(2 * k - n), k))

    def load(b, pg):
        start = pg * ROWS if isinstance(pg, int) else pl.multiple_of(pg * ROWS, ROWS)
        return pltpu.make_async_copy(
            echoes.at[0, :, b, pl.ds(start, ROWS), :], xin.at[b, pg], in_sem.at[b, pg]
        )

    for b in range(beams):
        for pg in range(groups):
            load(b, pg).start()
    table_copy = pltpu.make_async_copy(doppler_hbm, table, table_sem)
    table_copy.start()

    barrier = pltpu.get_barrier_semaphore()
    for k in order:
        pl.semaphore_signal(
            barrier, inc=1, device_id={"shard": lax.rem(me + k, n)}, device_id_type=MESH
        )

    rows = lax.broadcasted_iota(jnp.int32, (3 * GB, GB), 0) - GB
    cols = lax.broadcasted_iota(jnp.int32, (3 * GB, GB), 1)
    apart = jnp.abs(rows - cols)
    for b in range(beams):
        inside = (apart > guard[b]) & (apart <= guard[b] + train[b])
        band[b] = jnp.where(inside, 1.0, 0.0).astype(jnp.bfloat16)

    pl.semaphore_wait(barrier, n - 1)

    def compress(b, pg):
        load(b, pg).wait()
        for c in range(2):
            for i in range(ga):
                xs[c, i * ROWS:(i + 1) * ROWS, :] = xin[b, pg, c, :, i * GB:(i + 1) * GB]
        tc, ts = twiddle[0], twiddle[1]
        lhs = []
        for p in range(0, ROWS, 2):
            x = jnp.concatenate(
                [
                    jnp.concatenate([xs[c, pl.ds(p + e, ga, stride=ROWS), :] for c in range(2)], axis=0)
                    for e in range(2)
                ],
                axis=1,
            )
            y = dot(first[...], jnp.concatenate(parts(x), axis=0))
            y = y[:2 * ga] + y[2 * ga:]
            for e in range(2):
                yr, yi = y[:ga, e * GB:(e + 1) * GB], y[ga:, e * GB:(e + 1) * GB]
                z = jnp.concatenate([yr * tc + yi * ts, yi * tc - yr * ts], axis=1)
                high, low = parts(z)
                lhs.append(jnp.concatenate([high, low, high], axis=1))
        x = dot(jnp.concatenate(lhs, axis=0), second[...])
        lhs = []
        fr, fi = filt[0], filt[1]
        for p in range(ROWS):
            weight = taper[(me * groups + pg) * ROWS + p]
            hr, hi = fr * weight, fi * weight
            xr, xi = x[p * ga:(p + 1) * ga, :GB], x[p * ga:(p + 1) * ga, GB:]
            z = jnp.concatenate([xr * hr + xi * hi, xi * hr - xr * hi], axis=1)
            high, low = parts(z)
            lhs.append(jnp.concatenate([high, low, high], axis=1))
        x = dot(jnp.concatenate(lhs, axis=0), third[...])
        for p in range(0, ROWS, 2):
            pair = []
            for e in range(2):
                r = (p + e) * ga
                xr, xi = x[r:r + ga, :GB], x[r:r + ga, GB:]
                pair.append(jnp.concatenate([xr * tc - xi * ts, xi * tc + xr * ts], axis=0))
            y = dot(last[...], jnp.concatenate(parts(jnp.concatenate(pair, axis=1)), axis=0))
            y = y[:2 * ga] + y[2 * ga:]
            for e in range(2):
                for c in range(2):
                    sent.at[b, c, pg].reshape(ga * ROWS, GB)[pl.ds(p + e, ga, stride=ROWS), :] = y[
                        c * ga:(c + 1) * ga, e * GB:(e + 1) * GB
                    ]

    def send_group(b, pg):
        dst = got.at[b, :, :, me * groups + pg]
        for k in order:
            to = lax.rem(me + k, n)
            pltpu.make_async_remote_copy(
                src_ref=sent.at[b, :, pg, pl.ds(to * tiles, tiles)],
                dst_ref=dst,
                send_sem=send_sem.at[b],
                recv_sem=recv_sem.at[b, 0],
                device_id={"shard": to},
                device_id_type=MESH,
            ).start()
        pltpu.make_async_copy(
            sent.at[b, :, pg, pl.ds(me * tiles, tiles)], dst, recv_sem.at[b, 0]
        ).start()

    def send_tile(b, j):
        dst = got.at[b, :, j, pl.ds(me * groups, groups)]
        for k in order:
            to = lax.rem(me + k, n)
            pltpu.make_async_remote_copy(
                src_ref=sent.at[b, :, :, to * tiles + j],
                dst_ref=dst,
                send_sem=send_sem.at[b],
                recv_sem=recv_sem.at[b, j],
                device_id={"shard": to},
                device_id_type=MESH,
            ).start()
        pltpu.make_async_copy(sent.at[b, :, :, me * tiles + j], dst, recv_sem.at[b, j]).start()

    for b in range(beams):
        final = b == beams - 1

        @pl.loop(0, groups)
        def _(pg):
            compress(b, pg)
            if not final:
                send_group(b, pg)

        if final:
            @pl.loop(0, tiles)
            def _(t):
                send_tile(b, lax.rem(t * (tiles - 1), tiles))

    table_copy.wait()

    def transform(b, j):
        x = jnp.concatenate([got[b, c, j].reshape(pulses, GB) for c in range(2)], axis=1)
        high, low = parts(x)
        rhs[0:pulses] = high
        rhs[pulses:2 * pulses] = low
        rhs[2 * pulses:] = high
        spec[...] = dot(table[...], rhs[...])
        re = spec[:pulses, :GB] + spec[pulses:, GB:]
        im = spec[:pulses, GB:] - spec[pulses:, :GB]
        power[b, j] = re * re + im * im

    def edge_copy(b, side):
        to = lax.rem(me + (n - 1 if side == 0 else 1), n)
        return pltpu.make_async_remote_copy(
            src_ref=edge.at[b, side],
            dst_ref=halo.at[b, side],
            send_sem=edge_send.at[b, side],
            recv_sem=edge_recv.at[b, side],
            device_id={"shard": to},
            device_id_type=MESH,
        )

    def send_edges(b):
        edge[b, 0] = power[b, 0].T[:EDGE]
        edge[b, 1] = power[b, tiles - 1].T[GB - EDGE:]
        for side in range(2):
            edge_copy(b, side).start()

    def put(b, j):
        return pltpu.make_async_copy(
            result.at[b, j], out.at[0, b, :, pl.ds(pl.multiple_of(j * GB, GB), GB)], out_sem.at[b, j]
        )

    def cfar(b):
        for side in range(2):
            edge_copy(b, side).wait()
        zeros = jnp.zeros((GB - EDGE, pulses), jnp.float32)
        after = jnp.concatenate([jnp.where(me < n - 1, halo[b, 0], 0.0), zeros], axis=0).T
        before = jnp.concatenate([zeros, jnp.where(me > 0, halo[b, 1], 0.0)], axis=0).T
        twice = 2.0 * train[b].astype(jnp.float32)
        base = floor[b] * twice
        for j in range(tiles):
            here = power[b, j]
            near = jnp.concatenate(
                [
                    power[b, j - 1] if j else before,
                    here,
                    power[b, j + 1] if j < tiles - 1 else after,
                ],
                axis=1,
            )
            high, low = parts(near)
            total = dot(high, band[b]) + dot(low, band[b])
            result[b, j] = here * twice / (base + total)
            put(b, j).start()

    for b in range(beams):
        if b < beams - 1:
            pltpu.make_async_copy(got.at[b], got.at[b], recv_sem.at[b, 0]).wait()

            @pl.loop(0, tiles)
            def _(j):
                transform(b, j)

            send_edges(b)
            cfar(b)
        else:
            for t in range(tiles):
                j = t * (tiles - 1) % tiles
                arrived = got.at[b, :, j]
                pltpu.make_async_copy(arrived, arrived, recv_sem.at[b, j]).wait()
                transform(b, j)
                if t == min(1, tiles - 1):
                    send_edges(b)
            cfar(b)

    for b in range(beams):
        whole = sent.at[b, :, :, pl.ds(0, (n - 1) * tiles)]
        pltpu.make_async_copy(whole, whole, send_sem.at[b]).wait()
        for j in range(tiles):
            put(b, j).wait()


def solution(mesh):
    n = mesh.shape["shard"]

    def step(echoes, waveform, doppler_taper, cfar_guard, cfar_train, noise_floor):
        beams, local, gates = echoes.shape[2:]
        pulses = local * n
        ga = gates // GB
        tiles = ga // n
        groups = local // ROWS
        scale = 1.0 / (gates * math.sqrt(pulses))
        filt = waveform.reshape(2, GB, ga).transpose(0, 2, 1) * scale
        consts = tables(gates, pulses)
        vmem = pl.BlockSpec(memory_space=pltpu.VMEM)
        smem = pl.BlockSpec(memory_space=pltpu.SMEM)
        hbm = pl.BlockSpec(memory_space=pl.ANY)
        f32, bf16 = jnp.float32, jnp.bfloat16
        dma = pltpu.SemaphoreType.DMA
        return pl.pallas_call(
            functools.partial(kernel, n, beams, pulses, gates),
            out_shape=jax.ShapeDtypeStruct((1, beams, pulses, gates // n), f32),
            in_specs=[hbm, vmem, smem, smem, smem, smem, vmem, vmem, vmem, vmem, vmem, hbm],
            out_specs=hbm,
            scratch_shapes=[
                pltpu.VMEM((beams, groups, 2, ROWS, gates), f32),
                pltpu.VMEM((2, ga * ROWS, GB), f32),
                pltpu.VMEM((beams, 2, groups, ga, ROWS, GB), f32),
                pltpu.VMEM((beams, 2, tiles, pulses // ROWS, ROWS, GB), f32),
                pltpu.VMEM((2 * pulses, 3 * pulses), bf16),
                pltpu.VMEM((3 * pulses, 2 * GB), bf16),
                pltpu.VMEM((2 * pulses, 2 * GB), f32),
                pltpu.VMEM((beams, tiles, pulses, GB), f32),
                pltpu.VMEM((beams, 2, EDGE, pulses), f32),
                pltpu.VMEM((beams, 2, EDGE, pulses), f32),
                pltpu.VMEM((beams, 3 * GB, GB), bf16),
                pltpu.VMEM((beams, tiles, pulses, GB), f32),
                dma((beams, groups)),
                dma,
                dma((beams,)),
                dma((beams, tiles)),
                dma((beams, 2)),
                dma((beams, 2)),
                dma((beams, tiles)),
            ],
            compiler_params=pltpu.CompilerParams(
                collective_id=0, has_side_effects=True, vmem_limit_bytes=60 * 1024 * 1024
            ),
        )(
            echoes, filt, doppler_taper, cfar_guard, cfar_train, noise_floor,
            *(jnp.asarray(c) for c in consts),
        )

    in_specs = (
        P(None, None, "groups", "shard", None),
        P(),
        P(),
        P("groups"),
        P("groups"),
        P("groups"),
    )
    return jax.shard_map(
        step, mesh=mesh, in_specs=in_specs, out_specs=P(None, "groups", None, "shard"), check_vma=False
    )
```

```python
import functools
import math

import jax
import jax.numpy as jnp
import numpy as np
from jax import lax
from jax.experimental import pallas as pl
from jax.experimental.pallas import tpu as pltpu
from jax.sharding import PartitionSpec as P

GB = 128
ROWS = 8
EDGE = 24
MESH = pl.DeviceIdType.MESH


def split(table):
    table = np.asarray(table, np.float32)
    high = table.astype(jnp.bfloat16)
    low = (table - high.astype(np.float32)).astype(jnp.bfloat16)
    return high, low


def dft(length, size=None):
    size = size or length
    i = np.arange(size)[:, None] * np.arange(length)[None, :] % length
    angles = 2.0 * np.pi / length * i
    return np.cos(angles), np.sin(angles)


def tables(gates, pulses):
    ga = gates // GB
    ca, sa = dft(ga)
    cb, sb = dft(GB)

    def left(matrix):
        high, low = split(matrix)
        return np.block([[high, high], [low, np.zeros_like(low)]])

    first = left(np.block([[ca, sa], [-sa, ca]]))
    last = left(np.block([[ca, -sa], [sa, ca]]))
    per = GB // ga
    c = np.arange(GB).reshape(GB // per, per).T.reshape(-1)
    cb, sb = cb[:, c], sb[:, c]
    second = np.stack(split(np.block([[cb, -sb], [sb, cb]])))
    third = np.stack(split(np.block([[cb.T, sb.T], [-sb.T, cb.T]])))
    i = np.arange(ga)[:, None] * np.arange(GB)[None, :] % gates
    twiddle = np.stack([np.cos(2 * np.pi / gates * i), np.sin(2 * np.pi / gates * i)])
    half = pulses // 2
    cp, sp = dft(pulses)
    doppler = [
        np.stack(split(np.concatenate([cp[e::2, :half], sp[e::2, :half]], axis=0))) for e in range(2)
    ]
    return first, second, third, last, twiddle.astype(np.float32), np.stack(doppler)


def parts(x):
    high = x.astype(jnp.bfloat16)
    low = (x - high.astype(jnp.float32)).astype(jnp.bfloat16)
    return high, low


def dot(a, b):
    return jnp.dot(a, b, preferred_element_type=jnp.float32)


def kernel(
    n, beams, pulses, gates,
    echoes, waveform, taper, first, second, third, last, twiddle, doppler_hbm,
    power_out, halo_out,
    xin, xs, wave, filt, sent, got, table, rhs, spec, power, edge, halo, border,
    in_sem, table_sem, send_sem, recv_sem, edge_send, edge_recv, power_sem, halo_sem,
):
    me = lax.axis_index("shard")
    ga = gates // GB
    tiles = ga // n
    groups = pulses // n // ROWS
    order = sorted(range(1, n), key=lambda k: (abs(2 * k - n), k))

    def load(b, pg):
        start = pg * ROWS if isinstance(pg, int) else pl.multiple_of(pg * ROWS, ROWS)
        return pltpu.make_async_copy(
            echoes.at[0, :, b, pl.ds(start, ROWS), :], xin.at[b, pg], in_sem.at[b, pg]
        )

    for b in range(beams):
        for pg in range(groups):
            load(b, pg).start()
    table_copy = pltpu.make_async_copy(doppler_hbm, table, table_sem)

    barrier = pltpu.get_barrier_semaphore()
    for k in order:
        pl.semaphore_signal(
            barrier, inc=1, device_id={"shard": lax.rem(me + k, n)}, device_id_type=MESH
        )

    per = GB // ga
    scale = 1.0 / (gates * math.sqrt(pulses))
    for c in range(2):
        for m in range(ga):
            wave[m:m + 1, :] = waveform[c:c + 1, m * GB:(m + 1) * GB]
        lines = wave[...] * scale
        turned = [lines] + [pltpu.roll(lines, GB - h * ga, axis=1) for h in range(1, per)]
        filt[c] = jnp.concatenate(turned, axis=0).T[:ga]

    def stacked(ref):
        return jnp.concatenate([ref[0], ref[0], ref[1]], axis=0)

    def compress(b, pg):
        load(b, pg).wait()
        for c in range(2):
            for i in range(ga):
                xs[c, i * ROWS:(i + 1) * ROWS, :] = xin[b, pg, c, :, i * GB:(i + 1) * GB]
        tc, ts = twiddle[0], twiddle[1]
        lhs = []
        for p in range(0, ROWS, 2):
            x = jnp.concatenate(
                [
                    jnp.concatenate([xs[c, pl.ds(p + e, ga, stride=ROWS), :] for c in range(2)], axis=0)
                    for e in range(2)
                ],
                axis=1,
            )
            y = dot(first[...], jnp.concatenate(parts(x), axis=0))
            y = y[:2 * ga] + y[2 * ga:]
            for e in range(2):
                yr, yi = y[:ga, e * GB:(e + 1) * GB], y[ga:, e * GB:(e + 1) * GB]
                z = jnp.concatenate([yr * tc + yi * ts, yi * tc - yr * ts], axis=1)
                high, low = parts(z)
                lhs.append(jnp.concatenate([high, low, high], axis=1))
        x = dot(jnp.concatenate(lhs, axis=0), stacked(second))
        lhs = []
        fr, fi = filt[0], filt[1]
        for p in range(ROWS):
            weight = taper[(me * groups + pg) * ROWS + p]
            hr, hi = fr * weight, fi * weight
            xr, xi = x[p * ga:(p + 1) * ga, :GB], x[p * ga:(p + 1) * ga, GB:]
            z = jnp.concatenate([xr * hr + xi * hi, xi * hr - xr * hi], axis=1)
            high, low = parts(z)
            lhs.append(jnp.concatenate([high, low, high], axis=1))
        x = dot(jnp.concatenate(lhs, axis=0), stacked(third))
        for p in range(0, ROWS, 2):
            pair = []
            for e in range(2):
                r = (p + e) * ga
                xr, xi = x[r:r + ga, :GB], x[r:r + ga, GB:]
                pair.append(jnp.concatenate([xr * tc - xi * ts, xi * tc + xr * ts], axis=0))
            y = dot(last[...], jnp.concatenate(parts(jnp.concatenate(pair, axis=1)), axis=0))
            y = y[:2 * ga] + y[2 * ga:]
            for e in range(2):
                for c in range(2):
                    sent.at[b, c, pg].reshape(ga * ROWS, GB)[pl.ds(p + e, ga, stride=ROWS), :] = y[
                        c * ga:(c + 1) * ga, e * GB:(e + 1) * GB
                    ]

    def send_group(b, pg):
        dst = got.at[b, :, :, me * groups + pg]
        for k in order:
            to = lax.rem(me + k, n)
            pltpu.make_async_remote_copy(
                src_ref=sent.at[b, :, pg, pl.ds(to * tiles, tiles)],
                dst_ref=dst,
                send_sem=send_sem.at[b],
                recv_sem=recv_sem.at[b, 0],
                device_id={"shard": to},
                device_id_type=MESH,
            ).start()
        pltpu.make_async_copy(
            sent.at[b, :, pg, pl.ds(me * tiles, tiles)], dst, recv_sem.at[b, 0]
        ).start()

    def send_tile(b, j):
        dst = got.at[b, :, j, pl.ds(me * groups, groups)]
        for k in order:
            to = lax.rem(me + k, n)
            pltpu.make_async_remote_copy(
                src_ref=sent.at[b, :, :, to * tiles + j],
                dst_ref=dst,
                send_sem=send_sem.at[b],
                recv_sem=recv_sem.at[b, j],
                device_id={"shard": to},
                device_id_type=MESH,
            ).start()
        pltpu.make_async_copy(sent.at[b, :, :, me * tiles + j], dst, recv_sem.at[b, j]).start()

    for b in range(beams):
        final = b == beams - 1

        @pl.loop(0, groups)
        def _(pg):
            compress(b, pg)
            if b == 0:
                @pl.when(pg == 0)
                def _():
                    table_copy.start()
                    pl.semaphore_wait(barrier, n - 1)

            if not final:
                send_group(b, pg)

        if final:
            @pl.loop(0, tiles)
            def _(t):
                send_tile(b, lax.rem(t * (tiles - 1), tiles))

    table_copy.wait()

    half = pulses // 2

    def transform(b, j):
        x = jnp.concatenate([got[b, c, j].reshape(pulses, GB) for c in range(2)], axis=1)
        for e, y in enumerate((x[:half] + x[half:], x[:half] - x[half:])):
            high, low = parts(y)
            rhs[e, 0:half] = high
            rhs[e, half:2 * half] = low
            rhs[e, 2 * half:] = high
        for e in range(2):
            lhs = jnp.concatenate([table[e, 0], table[e, 0], table[e, 1]], axis=1)
            spec[e] = dot(lhs, rhs[e])
            re = spec[e, :half, :GB] + spec[e, half:, GB:]
            im = spec[e, :half, GB:] - spec[e, half:, :GB]
            power.at[b, j][pl.ds(e, half, stride=2), :] = re * re + im * im
        put(b, j).start()

    def put(b, j):
        return pltpu.make_async_copy(power.at[b, j], power_out.at[b, j], power_sem.at[b, j])

    def put_halo(b):
        return pltpu.make_async_copy(border.at[b], halo_out.at[b], halo_sem.at[b])

    def edge_copy(b, side):
        to = lax.rem(me + (n - 1 if side == 0 else 1), n)
        return pltpu.make_async_remote_copy(
            src_ref=edge.at[b, side],
            dst_ref=halo.at[b, side],
            send_sem=edge_send.at[b, side],
            recv_sem=edge_recv.at[b, side],
            device_id={"shard": to},
            device_id_type=MESH,
        )

    def send_edges(b):
        edge[b, 0] = power[b, 0].T[:EDGE]
        edge[b, 1] = power[b, tiles - 1].T[GB - EDGE:]
        for side in range(2):
            edge_copy(b, side).start()

    def take_edges(b):
        for side in range(2):
            edge_copy(b, side).wait()
        border[b, 0] = jnp.where(me < n - 1, halo[b, 0], 0.0)
        border[b, 1] = jnp.where(me > 0, halo[b, 1], 0.0)
        put_halo(b).start()

    for b in range(beams - 1):
        pltpu.make_async_copy(got.at[b], got.at[b], recv_sem.at[b, 0]).wait()

        @pl.loop(0, tiles)
        def _(j):
            transform(b, j)

        send_edges(b)

    b = beams - 1
    for t in range(tiles):
        j = t * (tiles - 1) % tiles
        arrived = got.at[b, :, j]
        pltpu.make_async_copy(arrived, arrived, recv_sem.at[b, j]).wait()
        transform(b, j)
        if t == min(1, tiles - 1):
            send_edges(b)
        if t == max(tiles - 2, min(1, tiles - 1)):
            for i in range(beams):
                take_edges(i)

    for b in range(beams):
        whole = sent.at[b, :, :, pl.ds(0, (n - 1) * tiles)]
        pltpu.make_async_copy(whole, whole, send_sem.at[b]).wait()
        put_halo(b).wait()
        for j in range(tiles):
            put(b, j).wait()


def cfar_kernel(guard, train, floor, power, halo, out):
    b = pl.program_id(0)
    tiles, rows = power.shape[1:3]
    m = lax.broadcasted_iota(jnp.int32, (3 * GB, GB), 0) - GB
    k = lax.broadcasted_iota(jnp.int32, (3 * GB, GB), 1)
    apart = jnp.abs(m - k)
    inside = (apart > guard[b]) & (apart <= guard[b] + train[b])
    band = jnp.where(inside, 1.0, 0.0).astype(jnp.bfloat16)
    band = jnp.concatenate([band, band], axis=0)
    zeros = jnp.zeros((GB - EDGE, rows), jnp.float32)
    after = jnp.concatenate([halo[0, 0], zeros], axis=0).T
    before = jnp.concatenate([zeros, halo[0, 1]], axis=0).T
    twice = 2.0 * train[b].astype(jnp.float32)
    base = floor[b] * twice
    cells = [before] + [power[0, j] for j in range(tiles)] + [after]
    cells = [(x, *parts(x)) for x in cells]
    for j in range(tiles):
        near = cells[j:j + 3]
        total = dot(jnp.concatenate([x[1] for x in near] + [x[2] for x in near], axis=1), band)
        out[0, 0, :, j * GB:(j + 1) * GB] = near[1][0] * twice / (base + total)


def solution(mesh):
    n = mesh.shape["shard"]

    def step(echoes, waveform, doppler_taper, cfar_guard, cfar_train, noise_floor):
        beams, local, gates = echoes.shape[2:]
        pulses = local * n
        ga = gates // GB
        tiles = ga // n
        groups = local // ROWS
        consts = tables(gates, pulses)
        vmem = pl.BlockSpec(memory_space=pltpu.VMEM)
        smem = pl.BlockSpec(memory_space=pltpu.SMEM)
        hbm = pl.BlockSpec(memory_space=pltpu.HBM)
        f32, bf16 = jnp.float32, jnp.bfloat16
        dma = pltpu.SemaphoreType.DMA
        power, halo = pl.pallas_call(
            functools.partial(kernel, n, beams, pulses, gates),
            out_shape=(
                jax.ShapeDtypeStruct((beams, tiles, pulses, GB), f32),
                jax.ShapeDtypeStruct((beams, 2, EDGE, pulses), f32),
            ),
            in_specs=[hbm, vmem, smem, vmem, vmem, vmem, vmem, vmem, hbm],
            out_specs=(hbm, hbm),
            scratch_shapes=[
                pltpu.VMEM((beams, groups, 2, ROWS, gates), f32),
                pltpu.VMEM((2, ga * ROWS, GB), f32),
                pltpu.VMEM((ga, GB), f32),
                pltpu.VMEM((2, ga, GB), f32),
                pltpu.VMEM((beams, 2, groups, ga, ROWS, GB), f32),
                pltpu.VMEM((beams, 2, tiles, pulses // ROWS, ROWS, GB), f32),
                pltpu.VMEM((2, 2, pulses, pulses // 2), bf16),
                pltpu.VMEM((2, 3 * pulses // 2, 2 * GB), bf16),
                pltpu.VMEM((2, pulses, 2 * GB), f32),
                pltpu.VMEM((beams, tiles, pulses, GB), f32),
                pltpu.VMEM((beams, 2, EDGE, pulses), f32),
                pltpu.VMEM((beams, 2, EDGE, pulses), f32),
                pltpu.VMEM((beams, 2, EDGE, pulses), f32),
                dma((beams, groups)),
                dma,
                dma((beams,)),
                dma((beams, tiles)),
                dma((beams, 2)),
                dma((beams, 2)),
                dma((beams, tiles)),
                dma((beams,)),
            ],
            compiler_params=pltpu.CompilerParams(
                collective_id=0, has_side_effects=True, vmem_limit_bytes=60000 * 1024
            ),
        )(echoes, waveform, doppler_taper, *(jnp.asarray(c) for c in consts))
        cut = pulses // 2
        return pl.pallas_call(
            cfar_kernel,
            grid=(beams, pulses // cut),
            out_shape=jax.ShapeDtypeStruct((1, beams, pulses, gates // n), f32),
            in_specs=[
                smem, smem, smem,
                pl.BlockSpec((1, tiles, cut, GB), lambda b, q: (b, 0, q, 0)),
                pl.BlockSpec((1, 2, EDGE, cut), lambda b, q: (b, 0, 0, q)),
            ],
            out_specs=pl.BlockSpec((1, 1, cut, tiles * GB), lambda b, q: (0, b, q, 0)),
            compiler_params=pltpu.CompilerParams(vmem_limit_bytes=60000 * 1024),
        )(cfar_guard, cfar_train, noise_floor, power, halo)

    in_specs = (
        P(None, None, "groups", "shard", None),
        P(),
        P(),
        P("groups"),
        P("groups"),
        P("groups"),
    )
    return jax.shard_map(
        step, mesh=mesh, in_specs=in_specs, out_specs=P(None, "groups", None, "shard"), check_vma=False
    )
```

```python
import functools
import math

import jax
import jax.numpy as jnp
import numpy as np
from jax import lax
from jax.experimental import pallas as pl
from jax.experimental.pallas import tpu as pltpu
from jax.sharding import PartitionSpec as P

GB = 128
ROWS = 8
EDGE = 24
MESH = pl.DeviceIdType.MESH


def split(table):
    table = np.asarray(table, np.float32)
    high = table.astype(jnp.bfloat16)
    low = (table - high.astype(np.float32)).astype(jnp.bfloat16)
    return high, low


def dft(length, size=None):
    size = size or length
    i = np.arange(size)[:, None] * np.arange(length)[None, :] % length
    angles = 2.0 * np.pi / length * i
    return np.cos(angles), np.sin(angles)


def tables(gates, pulses):
    ga = gates // GB
    ca, sa = dft(ga)
    cb, sb = dft(GB)

    def left(matrix):
        high, low = split(matrix)
        return np.block([[high, high], [low, np.zeros_like(low)]])

    first = left(np.block([[ca, sa], [-sa, ca]]))
    last = left(np.block([[ca, -sa], [sa, ca]]))
    per = GB // ga
    c = np.arange(GB).reshape(GB // per, per).T.reshape(-1)
    cb, sb = cb[:, c], sb[:, c]
    second = np.stack(split(np.block([[cb, -sb], [sb, cb]])))
    third = np.stack(split(np.block([[cb.T, sb.T], [-sb.T, cb.T]])))
    i = np.arange(ga)[:, None] * np.arange(GB)[None, :] % gates
    twiddle = np.stack([np.cos(2 * np.pi / gates * i), np.sin(2 * np.pi / gates * i)])
    half = pulses // 2
    cp, sp = dft(pulses)
    doppler = [
        np.stack(split(np.concatenate([cp[e::2, :half], sp[e::2, :half]], axis=0))) for e in range(2)
    ]
    return first, second, third, last, twiddle.astype(np.float32), np.stack(doppler)


def parts(x):
    high = x.astype(jnp.bfloat16)
    low = (x - high.astype(jnp.float32)).astype(jnp.bfloat16)
    return high, low


def dot(a, b):
    return jnp.dot(a, b, preferred_element_type=jnp.float32)


def kernel(
    n, beams, pulses, gates,
    echoes, waveform, taper, first, second, third, last, twiddle, doppler_hbm,
    power_out, halo_out,
    xin, xs, wave, filt, sent, got, table, rhs, spec, power, edge, halo, border,
    in_sem, table_sem, send_sem, recv_sem, edge_send, edge_recv, power_sem, halo_sem,
):
    me = lax.axis_index("shard")
    ga = gates // GB
    tiles = ga // n
    groups = pulses // n // ROWS
    order = sorted(range(1, n), key=lambda k: (abs(2 * k - n), k))

    def load(b, pg):
        start = pg * ROWS if isinstance(pg, int) else pl.multiple_of(pg * ROWS, ROWS)
        return pltpu.make_async_copy(
            echoes.at[0, :, b, pl.ds(start, ROWS), :], xin.at[b, pg], in_sem.at[b, pg]
        )

    load(0, 0).start()
    table_copy = pltpu.make_async_copy(doppler_hbm, table, table_sem)

    barrier = pltpu.get_barrier_semaphore()
    for k in order:
        pl.semaphore_signal(
            barrier, inc=1, device_id={"shard": lax.rem(me + k, n)}, device_id_type=MESH
        )

    per = GB // ga
    scale = 1.0 / (gates * math.sqrt(pulses))
    for c in range(2):
        for m in range(ga):
            wave[m:m + 1, :] = waveform[c:c + 1, m * GB:(m + 1) * GB]
        lines = wave[...] * scale
        turned = [lines] + [pltpu.roll(lines, GB - h * ga, axis=1) for h in range(1, per)]
        filt[c] = jnp.concatenate(turned, axis=0).T[:ga]

    def stacked(ref):
        return jnp.concatenate([ref[0], ref[0], ref[1]], axis=0)

    def load_rest():
        for b in range(beams):
            for pg in range(groups):
                if (b, pg) != (0, 0):
                    load(b, pg).start()
        table_copy.start()

    def compress(b, pg):
        load(b, pg).wait()
        if b == 0:
            pl.when(pg == 0)(load_rest)
        for c in range(2):
            for i in range(ga):
                xs[c, i * ROWS:(i + 1) * ROWS, :] = xin[b, pg, c, :, i * GB:(i + 1) * GB]
        tc, ts = twiddle[0], twiddle[1]
        lhs = []
        for p in range(0, ROWS, 2):
            x = jnp.concatenate(
                [
                    jnp.concatenate([xs[c, pl.ds(p + e, ga, stride=ROWS), :] for c in range(2)], axis=0)
                    for e in range(2)
                ],
                axis=1,
            )
            y = dot(first[...], jnp.concatenate(parts(x), axis=0))
            y = y[:2 * ga] + y[2 * ga:]
            for e in range(2):
                yr, yi = y[:ga, e * GB:(e + 1) * GB], y[ga:, e * GB:(e + 1) * GB]
                z = jnp.concatenate([yr * tc + yi * ts, yi * tc - yr * ts], axis=1)
                high, low = parts(z)
                lhs.append(jnp.concatenate([high, low, high], axis=1))
        x = dot(jnp.concatenate(lhs, axis=0), stacked(second))
        lhs = []
        fr, fi = filt[0], filt[1]
        for p in range(ROWS):
            weight = taper[(me * groups + pg) * ROWS + p]
            hr, hi = fr * weight, fi * weight
            xr, xi = x[p * ga:(p + 1) * ga, :GB], x[p * ga:(p + 1) * ga, GB:]
            z = jnp.concatenate([xr * hr + xi * hi, xi * hr - xr * hi], axis=1)
            high, low = parts(z)
            lhs.append(jnp.concatenate([high, low, high], axis=1))
        x = dot(jnp.concatenate(lhs, axis=0), stacked(third))
        for p in range(0, ROWS, 2):
            pair = []
            for e in range(2):
                r = (p + e) * ga
                xr, xi = x[r:r + ga, :GB], x[r:r + ga, GB:]
                pair.append(jnp.concatenate([xr * tc - xi * ts, xi * tc + xr * ts], axis=0))
            y = dot(last[...], jnp.concatenate(parts(jnp.concatenate(pair, axis=1)), axis=0))
            y = y[:2 * ga] + y[2 * ga:]
            for e in range(2):
                for c in range(2):
                    sent.at[b, c, pg].reshape(ga * ROWS, GB)[pl.ds(p + e, ga, stride=ROWS), :] = y[
                        c * ga:(c + 1) * ga, e * GB:(e + 1) * GB
                    ]

    def send_group(b, pg):
        dst = got.at[b, :, :, me * groups + pg]
        for k in order:
            to = lax.rem(me + k, n)
            pltpu.make_async_remote_copy(
                src_ref=sent.at[b, :, pg, pl.ds(to * tiles, tiles)],
                dst_ref=dst,
                send_sem=send_sem.at[b],
                recv_sem=recv_sem.at[b, 0],
                device_id={"shard": to},
                device_id_type=MESH,
            ).start()
        pltpu.make_async_copy(
            sent.at[b, :, pg, pl.ds(me * tiles, tiles)], dst, recv_sem.at[b, 0]
        ).start()

    def send_tile(b, j):
        dst = got.at[b, :, j, pl.ds(me * groups, groups)]
        for k in order:
            to = lax.rem(me + k, n)
            pltpu.make_async_remote_copy(
                src_ref=sent.at[b, :, :, to * tiles + j],
                dst_ref=dst,
                send_sem=send_sem.at[b],
                recv_sem=recv_sem.at[b, j],
                device_id={"shard": to},
                device_id_type=MESH,
            ).start()
        pltpu.make_async_copy(sent.at[b, :, :, me * tiles + j], dst, recv_sem.at[b, j]).start()

    for b in range(beams):
        final = b == beams - 1

        @pl.loop(0, groups)
        def _(pg):
            compress(b, pg)
            if b == 0:
                @pl.when(pg == 0)
                def _():
                    pl.semaphore_wait(barrier, n - 1)

            if not final:
                send_group(b, pg)

        if final:
            @pl.loop(0, tiles)
            def _(t):
                send_tile(b, lax.rem(t * (tiles - 1), tiles))

    table_copy.wait()

    half = pulses // 2

    def transform(b, j):
        x = jnp.concatenate([got[b, c, j].reshape(pulses, GB) for c in range(2)], axis=1)
        for e, y in enumerate((x[:half] + x[half:], x[:half] - x[half:])):
            high, low = parts(y)
            rhs[e, 0:half] = high
            rhs[e, half:2 * half] = low
            rhs[e, 2 * half:] = high
        for e in range(2):
            lhs = jnp.concatenate([table[e, 0], table[e, 0], table[e, 1]], axis=1)
            spec[e] = dot(lhs, rhs[e])
            re = spec[e, :half, :GB] + spec[e, half:, GB:]
            im = spec[e, :half, GB:] - spec[e, half:, :GB]
            power.at[b, j][pl.ds(e, half, stride=2), :] = re * re + im * im
        put(b, j).start()

    def put(b, j):
        return pltpu.make_async_copy(power.at[b, j], power_out.at[b, j], power_sem.at[b, j])

    def put_halo(b):
        return pltpu.make_async_copy(border.at[b], halo_out.at[b], halo_sem.at[b])

    def edge_copy(b, side):
        to = lax.rem(me + (n - 1 if side == 0 else 1), n)
        return pltpu.make_async_remote_copy(
            src_ref=edge.at[b, side],
            dst_ref=halo.at[b, side],
            send_sem=edge_send.at[b, side],
            recv_sem=edge_recv.at[b, side],
            device_id={"shard": to},
            device_id_type=MESH,
        )

    def send_edges(b):
        edge[b, 0] = power[b, 0].T[:EDGE]
        edge[b, 1] = power[b, tiles - 1].T[GB - EDGE:]
        for side in range(2):
            edge_copy(b, side).start()

    def take_edges(b):
        for side in range(2):
            edge_copy(b, side).wait()
        border[b, 0] = jnp.where(me < n - 1, halo[b, 0], 0.0)
        border[b, 1] = jnp.where(me > 0, halo[b, 1], 0.0)
        put_halo(b).start()

    for b in range(beams - 1):
        pltpu.make_async_copy(got.at[b], got.at[b], recv_sem.at[b, 0]).wait()

        @pl.loop(0, tiles)
        def _(j):
            transform(b, j)

        send_edges(b)

    b = beams - 1
    for t in range(tiles):
        j = t * (tiles - 1) % tiles
        arrived = got.at[b, :, j]
        pltpu.make_async_copy(arrived, arrived, recv_sem.at[b, j]).wait()
        transform(b, j)
        if t == min(1, tiles - 1):
            send_edges(b)
        if t == max(tiles - 2, min(1, tiles - 1)):
            for i in range(beams):
                take_edges(i)

    for b in range(beams):
        whole = sent.at[b, :, :, pl.ds(0, (n - 1) * tiles)]
        pltpu.make_async_copy(whole, whole, send_sem.at[b]).wait()
        put_halo(b).wait()
        for j in range(tiles):
            put(b, j).wait()


def cfar_kernel(guard, train, floor, power, halo, out):
    b = pl.program_id(0)
    tiles, rows = power.shape[1:3]
    span = 2 if tiles % 2 == 0 else 1
    m = lax.broadcasted_iota(jnp.int32, ((span + 2) * GB, span * GB), 0) - GB
    k = lax.broadcasted_iota(jnp.int32, ((span + 2) * GB, span * GB), 1)
    apart = jnp.abs(m - k)
    inside = (apart > guard[b]) & (apart <= guard[b] + train[b])
    band = jnp.where(inside, 1.0, 0.0).astype(jnp.bfloat16)
    band = jnp.concatenate([band, band], axis=0)
    zeros = jnp.zeros((GB - EDGE, rows), jnp.float32)
    after = jnp.concatenate([halo[0, 0], zeros], axis=0).T
    before = jnp.concatenate([zeros, halo[0, 1]], axis=0).T
    twice = 2.0 * train[b].astype(jnp.float32)
    base = floor[b] * twice
    cells = [before] + [power[0, j] for j in range(tiles)] + [after]
    cells = [(x, *parts(x)) for x in cells]
    for j in range(0, tiles, span):
        near = cells[j:j + span + 2]
        total = dot(jnp.concatenate([x[1] for x in near] + [x[2] for x in near], axis=1), band)
        for i in range(span):
            here = near[1 + i][0]
            out[0, 0, :, (j + i) * GB:(j + i + 1) * GB] = (
                here * twice / (base + total[:, i * GB:(i + 1) * GB])
            )


def solution(mesh):
    n = mesh.shape["shard"]

    def step(echoes, waveform, doppler_taper, cfar_guard, cfar_train, noise_floor):
        beams, local, gates = echoes.shape[2:]
        pulses = local * n
        ga = gates // GB
        tiles = ga // n
        groups = local // ROWS
        consts = tables(gates, pulses)
        vmem = pl.BlockSpec(memory_space=pltpu.VMEM)
        smem = pl.BlockSpec(memory_space=pltpu.SMEM)
        hbm = pl.BlockSpec(memory_space=pltpu.HBM)
        f32, bf16 = jnp.float32, jnp.bfloat16
        dma = pltpu.SemaphoreType.DMA
        power, halo = pl.pallas_call(
            functools.partial(kernel, n, beams, pulses, gates),
            out_shape=(
                jax.ShapeDtypeStruct((beams, tiles, pulses, GB), f32),
                jax.ShapeDtypeStruct((beams, 2, EDGE, pulses), f32),
            ),
            in_specs=[hbm, vmem, smem, vmem, vmem, vmem, vmem, vmem, hbm],
            out_specs=(hbm, hbm),
            scratch_shapes=[
                pltpu.VMEM((beams, groups, 2, ROWS, gates), f32),
                pltpu.VMEM((2, ga * ROWS, GB), f32),
                pltpu.VMEM((ga, GB), f32),
                pltpu.VMEM((2, ga, GB), f32),
                pltpu.VMEM((beams, 2, groups, ga, ROWS, GB), f32),
                pltpu.VMEM((beams, 2, tiles, pulses // ROWS, ROWS, GB), f32),
                pltpu.VMEM((2, 2, pulses, pulses // 2), bf16),
                pltpu.VMEM((2, 3 * pulses // 2, 2 * GB), bf16),
                pltpu.VMEM((2, pulses, 2 * GB), f32),
                pltpu.VMEM((beams, tiles, pulses, GB), f32),
                pltpu.VMEM((beams, 2, EDGE, pulses), f32),
                pltpu.VMEM((beams, 2, EDGE, pulses), f32),
                pltpu.VMEM((beams, 2, EDGE, pulses), f32),
                dma((beams, groups)),
                dma,
                dma((beams,)),
                dma((beams, tiles)),
                dma((beams, 2)),
                dma((beams, 2)),
                dma((beams, tiles)),
                dma((beams,)),
            ],
            compiler_params=pltpu.CompilerParams(
                collective_id=0, has_side_effects=True, vmem_limit_bytes=60000 * 1024
            ),
        )(echoes, waveform, doppler_taper, *(jnp.asarray(c) for c in consts))
        cut = pulses // 4
        return pl.pallas_call(
            cfar_kernel,
            grid=(beams, pulses // cut),
            out_shape=jax.ShapeDtypeStruct((1, beams, pulses, gates // n), f32),
            in_specs=[
                smem, smem, smem,
                pl.BlockSpec((1, tiles, cut, GB), lambda b, q: (b, 0, q, 0)),
                pl.BlockSpec((1, 2, EDGE, cut), lambda b, q: (b, 0, 0, q)),
            ],
            out_specs=pl.BlockSpec((1, 1, cut, tiles * GB), lambda b, q: (0, b, q, 0)),
            compiler_params=pltpu.CompilerParams(vmem_limit_bytes=60000 * 1024),
        )(cfar_guard, cfar_train, noise_floor, power, halo)

    in_specs = (
        P(None, None, "groups", "shard", None),
        P(),
        P(),
        P("groups"),
        P("groups"),
        P("groups"),
    )
    return jax.shard_map(
        step, mesh=mesh, in_specs=in_specs, out_specs=P(None, "groups", None, "shard"), check_vma=False
    )
```

```python
import functools
import math

import jax
import jax.numpy as jnp
import numpy as np
from jax import lax
from jax.experimental import pallas as pl
from jax.experimental.pallas import tpu as pltpu
from jax.sharding import PartitionSpec as P

GB = 128
ROWS = 8
EDGE = 24
MESH = pl.DeviceIdType.MESH


def split(table):
    table = np.asarray(table, np.float32)
    high = table.astype(jnp.bfloat16)
    low = (table - high.astype(np.float32)).astype(jnp.bfloat16)
    return high, low


def dft(length, size=None):
    size = size or length
    i = np.arange(size)[:, None] * np.arange(length)[None, :] % length
    angles = 2.0 * np.pi / length * i
    return np.cos(angles), np.sin(angles)


def tables(gates, pulses):
    ga = gates // GB
    ca, sa = dft(ga)
    cb, sb = dft(GB)

    def left(matrix):
        high, low = split(matrix)
        return np.block([[high, high], [low, np.zeros_like(low)]])

    first = left(np.block([[ca, sa], [-sa, ca]]))
    last = left(np.block([[ca, -sa], [sa, ca]]))
    per = GB // ga
    c = np.arange(GB).reshape(GB // per, per).T.reshape(-1)
    cb, sb = cb[:, c], sb[:, c]
    second = np.stack(split(np.block([[cb, -sb], [sb, cb]])))
    third = np.stack(split(np.block([[cb.T, sb.T], [-sb.T, cb.T]])))
    i = np.arange(ga)[:, None] * np.arange(GB)[None, :] % gates
    twiddle = np.stack([np.cos(2 * np.pi / gates * i), np.sin(2 * np.pi / gates * i)])
    half = pulses // 2
    cp, sp = dft(pulses)
    doppler = [
        np.stack(split(np.concatenate([cp[e::2, :half], sp[e::2, :half]], axis=0))) for e in range(2)
    ]
    return first, second, third, last, twiddle.astype(np.float32), np.stack(doppler)


def parts(x):
    high = x.astype(jnp.bfloat16)
    low = (x - high.astype(jnp.float32)).astype(jnp.bfloat16)
    return high, low


def dot(a, b):
    return jnp.dot(a, b, preferred_element_type=jnp.float32)


def kernel(
    n, beams, pulses, gates,
    echoes, waveform, taper, first, second, third, last, twiddle, doppler_hbm,
    power_out, halo_out,
    xin, xs, wave, filt, sent, got, table, rhs, spec, power, edge, halo, border,
    in_sem, table_sem, send_sem, recv_sem, edge_send, edge_recv, power_sem, halo_sem,
):
    me = lax.axis_index("shard")
    ga = gates // GB
    tiles = ga // n
    groups = pulses // n // ROWS
    order = sorted(range(1, n), key=lambda k: (abs(2 * k - n), k))

    def load(b, pg):
        start = pg * ROWS if isinstance(pg, int) else pl.multiple_of(pg * ROWS, ROWS)
        return pltpu.make_async_copy(
            echoes.at[0, :, b, pl.ds(start, ROWS), :], xin.at[b, pg], in_sem.at[b, pg]
        )

    load(0, 0).start()
    table_copy = pltpu.make_async_copy(doppler_hbm, table, table_sem)

    barrier = pltpu.get_barrier_semaphore()
    for k in order:
        pl.semaphore_signal(
            barrier, inc=1, device_id={"shard": lax.rem(me + k, n)}, device_id_type=MESH
        )

    per = GB // ga
    scale = 1.0 / (gates * math.sqrt(pulses))
    for c in range(2):
        for m in range(ga):
            wave[m:m + 1, :] = waveform[c:c + 1, m * GB:(m + 1) * GB]
        lines = wave[...] * scale
        turned = [lines] + [pltpu.roll(lines, GB - h * ga, axis=1) for h in range(1, per)]
        filt[c] = jnp.concatenate(turned, axis=0).T[:ga]

    def stacked(ref):
        return jnp.concatenate([ref[0], ref[0], ref[1]], axis=0)

    def load_rest():
        for b in range(beams):
            for pg in range(groups):
                if (b, pg) != (0, 0):
                    load(b, pg).start()
        table_copy.start()

    def compress(b, pg):
        load(b, pg).wait()
        if b == 0:
            pl.when(pg == 0)(load_rest)
        for c in range(2):
            for i in range(ga):
                xs[c, i * ROWS:(i + 1) * ROWS, :] = xin[b, pg, c, :, i * GB:(i + 1) * GB]
        tc, ts = twiddle[0], twiddle[1]
        lhs = []
        for p in range(0, ROWS, 2):
            x = jnp.concatenate(
                [
                    jnp.concatenate([xs[c, pl.ds(p + e, ga, stride=ROWS), :] for c in range(2)], axis=0)
                    for e in range(2)
                ],
                axis=1,
            )
            y = dot(first[...], jnp.concatenate(parts(x), axis=0))
            y = y[:2 * ga] + y[2 * ga:]
            for e in range(2):
                yr, yi = y[:ga, e * GB:(e + 1) * GB], y[ga:, e * GB:(e + 1) * GB]
                z = jnp.concatenate([yr * tc + yi * ts, yi * tc - yr * ts], axis=1)
                high, low = parts(z)
                lhs.append(jnp.concatenate([high, low, high], axis=1))
        x = dot(jnp.concatenate(lhs, axis=0), stacked(second))
        lhs = []
        fr, fi = filt[0], filt[1]
        for p in range(ROWS):
            weight = taper[(me * groups + pg) * ROWS + p]
            hr, hi = fr * weight, fi * weight
            xr, xi = x[p * ga:(p + 1) * ga, :GB], x[p * ga:(p + 1) * ga, GB:]
            z = jnp.concatenate([xr * hr + xi * hi, xi * hr - xr * hi], axis=1)
            high, low = parts(z)
            lhs.append(jnp.concatenate([high, low, high], axis=1))
        x = dot(jnp.concatenate(lhs, axis=0), stacked(third))
        for p in range(0, ROWS, 2):
            pair = []
            for e in range(2):
                r = (p + e) * ga
                xr, xi = x[r:r + ga, :GB], x[r:r + ga, GB:]
                pair.append(jnp.concatenate([xr * tc - xi * ts, xi * tc + xr * ts], axis=0))
            y = dot(last[...], jnp.concatenate(parts(jnp.concatenate(pair, axis=1)), axis=0))
            y = y[:2 * ga] + y[2 * ga:]
            for e in range(2):
                for c in range(2):
                    sent.at[b, c, pg].reshape(ga * ROWS, GB)[pl.ds(p + e, ga, stride=ROWS), :] = y[
                        c * ga:(c + 1) * ga, e * GB:(e + 1) * GB
                    ]

    def send_group(b, pg):
        dst = got.at[b, :, :, me * groups + pg]
        for k in order:
            to = lax.rem(me + k, n)
            pltpu.make_async_remote_copy(
                src_ref=sent.at[b, :, pg, pl.ds(to * tiles, tiles)],
                dst_ref=dst,
                send_sem=send_sem.at[b],
                recv_sem=recv_sem.at[b, 0],
                device_id={"shard": to},
                device_id_type=MESH,
            ).start()
        pltpu.make_async_copy(
            sent.at[b, :, pg, pl.ds(me * tiles, tiles)], dst, recv_sem.at[b, 0]
        ).start()

    def send_tile(b, j):
        dst = got.at[b, :, j, pl.ds(me * groups, groups)]
        for k in order:
            to = lax.rem(me + k, n)
            pltpu.make_async_remote_copy(
                src_ref=sent.at[b, :, :, to * tiles + j],
                dst_ref=dst,
                send_sem=send_sem.at[b],
                recv_sem=recv_sem.at[b, j],
                device_id={"shard": to},
                device_id_type=MESH,
            ).start()
        pltpu.make_async_copy(sent.at[b, :, :, me * tiles + j], dst, recv_sem.at[b, j]).start()

    for b in range(beams):
        final = b == beams - 1

        @pl.loop(0, groups)
        def _(pg):
            compress(b, pg)
            if b == 0:
                @pl.when(pg == 0)
                def _():
                    pl.semaphore_wait(barrier, n - 1)

            if not final:
                send_group(b, pg)

        if final:
            @pl.loop(0, tiles)
            def _(t):
                send_tile(b, lax.rem(t * (tiles - 1), tiles))

    table_copy.wait()

    half = pulses // 2

    def transform(b, j):
        x = jnp.concatenate([got[b, c, j].reshape(pulses, GB) for c in range(2)], axis=1)
        for e, y in enumerate((x[:half] + x[half:], x[:half] - x[half:])):
            high, low = parts(y)
            rhs[e, 0:half] = high
            rhs[e, half:2 * half] = low
            rhs[e, 2 * half:] = high
        for e in range(2):
            lhs = jnp.concatenate([table[e, 0], table[e, 0], table[e, 1]], axis=1)
            spec[e] = dot(lhs, rhs[e])
            re = spec[e, :half, :GB] + spec[e, half:, GB:]
            im = spec[e, :half, GB:] - spec[e, half:, :GB]
            power.at[b, j][pl.ds(e, half, stride=2), :] = re * re + im * im
        put(b, j).start()

    def put(b, j):
        return pltpu.make_async_copy(power.at[b, j], power_out.at[b, j], power_sem.at[b, j])

    def put_halo(b):
        return pltpu.make_async_copy(border.at[b], halo_out.at[b], halo_sem.at[b])

    def edge_copy(b, side):
        to = lax.rem(me + (n - 1 if side == 0 else 1), n)
        return pltpu.make_async_remote_copy(
            src_ref=edge.at[b, side],
            dst_ref=halo.at[b, side],
            send_sem=edge_send.at[b, side],
            recv_sem=edge_recv.at[b, side],
            device_id={"shard": to},
            device_id_type=MESH,
        )

    def send_edges(b):
        edge[b, 0] = power[b, 0].T[:EDGE]
        edge[b, 1] = power[b, tiles - 1].T[GB - EDGE:]
        for side in range(2):
            edge_copy(b, side).start()

    def take_edges(b):
        for side in range(2):
            edge_copy(b, side).wait()
        border[b, 0] = jnp.where(me < n - 1, halo[b, 0], 0.0)
        border[b, 1] = jnp.where(me > 0, halo[b, 1], 0.0)
        put_halo(b).start()

    for b in range(beams - 1):
        pltpu.make_async_copy(got.at[b], got.at[b], recv_sem.at[b, 0]).wait()

        @pl.loop(0, tiles)
        def _(j):
            transform(b, j)

        send_edges(b)

    b = beams - 1
    for t in range(tiles):
        j = t * (tiles - 1) % tiles
        arrived = got.at[b, :, j]
        pltpu.make_async_copy(arrived, arrived, recv_sem.at[b, j]).wait()
        transform(b, j)
        if t == min(1, tiles - 1):
            send_edges(b)
        if t == max(tiles - 2, min(1, tiles - 1)):
            for i in range(beams):
                take_edges(i)

    for b in range(beams):
        whole = sent.at[b, :, :, pl.ds(0, (n - 1) * tiles)]
        pltpu.make_async_copy(whole, whole, send_sem.at[b]).wait()
        put_halo(b).wait()
        for j in range(tiles):
            put(b, j).wait()


def cfar_kernel(guard, train, floor, power, halo, out):
    b = pl.program_id(0)
    tiles, rows = power.shape[1:3]
    span = 1
    m = lax.broadcasted_iota(jnp.int32, ((span + 2) * GB, span * GB), 0) - GB
    k = lax.broadcasted_iota(jnp.int32, ((span + 2) * GB, span * GB), 1)
    apart = jnp.abs(m - k)
    inside = (apart > guard[b]) & (apart <= guard[b] + train[b])
    band = jnp.where(inside, 1.0, 0.0).astype(jnp.bfloat16)
    band = jnp.concatenate([band, band], axis=0)
    zeros = jnp.zeros((GB - EDGE, rows), jnp.float32)
    after = jnp.concatenate([halo[0, 0], zeros], axis=0).T
    before = jnp.concatenate([zeros, halo[0, 1]], axis=0).T
    twice = 2.0 * train[b].astype(jnp.float32)
    base = floor[b] * twice
    cells = [before] + [power[0, j] for j in range(tiles)] + [after]
    cells = [(x, *parts(x)) for x in cells]
    for j in range(0, tiles, span):
        near = cells[j:j + span + 2]
        total = dot(jnp.concatenate([x[1] for x in near] + [x[2] for x in near], axis=1), band)
        for i in range(span):
            here = near[1 + i][0]
            out[0, 0, :, (j + i) * GB:(j + i + 1) * GB] = (
                here * twice / (base + total[:, i * GB:(i + 1) * GB])
            )


def solution(mesh):
    n = mesh.shape["shard"]

    def step(echoes, waveform, doppler_taper, cfar_guard, cfar_train, noise_floor):
        beams, local, gates = echoes.shape[2:]
        pulses = local * n
        ga = gates // GB
        tiles = ga // n
        groups = local // ROWS
        consts = tables(gates, pulses)
        vmem = pl.BlockSpec(memory_space=pltpu.VMEM)
        smem = pl.BlockSpec(memory_space=pltpu.SMEM)
        hbm = pl.BlockSpec(memory_space=pltpu.HBM)
        f32, bf16 = jnp.float32, jnp.bfloat16
        dma = pltpu.SemaphoreType.DMA
        power, halo = pl.pallas_call(
            functools.partial(kernel, n, beams, pulses, gates),
            out_shape=(
                jax.ShapeDtypeStruct((beams, tiles, pulses, GB), f32),
                jax.ShapeDtypeStruct((beams, 2, EDGE, pulses), f32),
            ),
            in_specs=[hbm, vmem, smem, vmem, vmem, vmem, vmem, vmem, hbm],
            out_specs=(hbm, hbm),
            scratch_shapes=[
                pltpu.VMEM((beams, groups, 2, ROWS, gates), f32),
                pltpu.VMEM((2, ga * ROWS, GB), f32),
                pltpu.VMEM((ga, GB), f32),
                pltpu.VMEM((2, ga, GB), f32),
                pltpu.VMEM((beams, 2, groups, ga, ROWS, GB), f32),
                pltpu.VMEM((beams, 2, tiles, pulses // ROWS, ROWS, GB), f32),
                pltpu.VMEM((2, 2, pulses, pulses // 2), bf16),
                pltpu.VMEM((2, 3 * pulses // 2, 2 * GB), bf16),
                pltpu.VMEM((2, pulses, 2 * GB), f32),
                pltpu.VMEM((beams, tiles, pulses, GB), f32),
                pltpu.VMEM((beams, 2, EDGE, pulses), f32),
                pltpu.VMEM((beams, 2, EDGE, pulses), f32),
                pltpu.VMEM((beams, 2, EDGE, pulses), f32),
                dma((beams, groups)),
                dma,
                dma((beams,)),
                dma((beams, tiles)),
                dma((beams, 2)),
                dma((beams, 2)),
                dma((beams, tiles)),
                dma((beams,)),
            ],
            compiler_params=pltpu.CompilerParams(
                collective_id=0, has_side_effects=True, vmem_limit_bytes=60000 * 1024
            ),
        )(echoes, waveform, doppler_taper, *(jnp.asarray(c) for c in consts))
        cut = pulses // 2
        return pl.pallas_call(
            cfar_kernel,
            grid=(beams, pulses // cut),
            out_shape=jax.ShapeDtypeStruct((1, beams, pulses, gates // n), f32),
            in_specs=[
                smem, smem, smem,
                pl.BlockSpec((1, tiles, cut, GB), lambda b, q: (b, 0, q, 0)),
                pl.BlockSpec((1, 2, EDGE, cut), lambda b, q: (b, 0, 0, q)),
            ],
            out_specs=pl.BlockSpec((1, 1, cut, tiles * GB), lambda b, q: (0, b, q, 0)),
            compiler_params=pltpu.CompilerParams(vmem_limit_bytes=60000 * 1024),
        )(cfar_guard, cfar_train, noise_floor, power, halo)

    in_specs = (
        P(None, None, "groups", "shard", None),
        P(),
        P(),
        P("groups"),
        P("groups"),
        P("groups"),
    )
    return jax.shard_map(
        step, mesh=mesh, in_specs=in_specs, out_specs=P(None, "groups", None, "shard"), check_vma=False
    )
```
